32 devices in a mesh: batch: 16 (over z, x, core), rep: 2 (over y).
Axes of the slice: x: 2, y: 2, z: 4, core: 2. Of those that a mesh axis runs over, the one named last changes fastest.
Arguments:
- behav_ids: int32 [512, 256], P(('batch', 'rep')), may hold values from 0 to 1023
- lengths: int32 [512], P(('batch', 'rep')), may hold values from 32 to 256
- cand_ids: int32 [512, 16], P(('batch', 'rep')), may hold values from 0 to 1023
- labels: int32 [512, 16], P(('batch', 'rep')), may hold values 0 or 1
- item_table: float32 [1024, 128], replicated, may hold values from -6 to 6
- att_behav: float32 [128, 80], replicated, may hold values from -0.5 to 0.5
- att_cand: float32 [128, 80], replicated, may hold values from -0.5 to 0.5
- att_bias: float32 [80], replicated, may hold values from -3 to 3
- att_out: float32 [80], replicated, may hold values from -0.625 to 0.625
- dense_in: float32 [512, 256], replicated, may hold values from -0.25 to 0.25
- dense_bias: float32 [256], replicated, may hold values from -3 to 3
- dense_out: float32 [256], replicated, may hold values from -0.375 to 0.375
Outputs:
- grad_table: float32 [1024, 128], replicated
- grad_att_behav: float32 [128, 80], replicated
- grad_att_cand: float32 [128, 80], replicated
- grad_att_bias: float32 [80], replicated
- grad_att_out: float32 [80], replicated
- grad_dense_in: float32 [512, 256], replicated
- grad_dense_bias: float32 [256], replicated
- grad_dense_out: float32 [256], replicated
- mean_loss: float32 [], replicated
The draws below stay inside these ranges and needn't reach their ends.
All inputs are finite; a program needn't handle non-finite values. No bound on the sum of `labels` on one device may be relied on, other than what follows from the above.
Results may differ from the reference program's by a relative error of at most 0.0003.
Values sent between devices are 32-bit elements; how exact they have to be, the bound alone decides.
No kernel may reach another device: no remote copies, remote signals or barrier semaphores. Data moves between devices by JAX's collectives and lax.ppermute only.
A program may use at most 64 MiB of HBM per device.

```python
import jax
import jax.numpy as jnp
from jax import lax

USERS_DEV = 16
CANDS = 16
SEQ = 256
E = 128
H = 80
FH = 256
CATS = 1024
FIN = 512
USERS = 512


def draw_behav_ids(key, part):
    first, second, third = jax.random.split(jax.random.fold_in(key, 17), 3)
    users = jnp.arange(USERS, dtype=jnp.int32)
    home = 2 * (users // USERS_DEV) % CATS
    picker = jax.random.randint(first, (USERS, SEQ), 0, 2)
    nearby = (home[:, None] + jax.random.randint(second, (USERS, SEQ), 0, 2)) % CATS
    spread = jax.random.randint(third, (USERS, SEQ), 0, CATS)
    return jnp.where(picker == 1, nearby, spread).astype(jnp.int32)


def with_ends(entries, key, low, high):
    place = [jax.random.randint(jax.random.fold_in(key, axis), (), 0, length) for axis, length in enumerate(entries.shape)]
    longest = entries.shape.index(max(entries.shape))
    neighbour = place[:longest] + [(place[longest] + 1) % entries.shape[longest]] + place[longest + 1:]
    return entries.at[tuple(place)].set(low).at[tuple(neighbour)].set(high)


def centred(key, shape, scale, most, kind=jnp.bfloat16):
    drawn = scale * jax.random.normal(key, shape, jnp.float32)
    return jnp.clip(drawn, min=-most, max=most).astype(kind)


def setup_inputs(seed: int = 0) -> dict:
    keys = jax.random.split(jax.random.key(seed), 13)
    return {
        "behav_ids": draw_behav_ids(jax.random.fold_in(keys[12], 71), 0),
        "lengths": with_ends(jax.random.randint(keys[1], (USERS,), SEQ // 8, SEQ + 1), jax.random.fold_in(keys[1], 1), SEQ // 8, SEQ).astype(jnp.int32),
        "cand_ids": with_ends(jax.random.randint(keys[2], (USERS, CANDS), 0, CATS), jax.random.fold_in(keys[2], 1), 0, CATS - 1).astype(jnp.int32),
        "labels": with_ends((jax.random.randint(keys[3], (USERS, CANDS), 0, 4) < 1).astype(jnp.int32), jax.random.fold_in(keys[3], 1), 0, 1),
        "item_table": centred(keys[4], (CATS, E), 1.0, 6.0, jnp.float32),
        "att_behav": centred(keys[5], (E, H), E ** -0.5, 0.5, jnp.float32),
        "att_cand": centred(keys[6], (E, H), E ** -0.5, 0.5, jnp.float32),
        "att_bias": centred(keys[7], (H,), 0.5, 3.0, jnp.float32),
        "att_out": centred(keys[8], (H,), H ** -0.5, 0.625, jnp.float32),
        "dense_in": centred(keys[9], (FIN, FH), FIN ** -0.5, 0.25, jnp.float32),
        "dense_bias": centred(keys[10], (FH,), 0.5, 3.0, jnp.float32),
        "dense_out": centred(keys[11], (FH,), FH ** -0.5, 0.375, jnp.float32),
    }


highest = lax.Precision.HIGHEST

def block_loss(item_table, att_behav, att_cand, att_bias, att_out, dense_in, dense_bias, dense_out, ids_block, lens_block, cands_block, labels_block):
    behaviors = item_table[ids_block]
    candidates = item_table[cands_block]
    places = jnp.arange(ids_block.shape[1], dtype=jnp.int32)
    live = (places[None, :] < lens_block[:, None]).astype(jnp.float32)
    pre_behav = jnp.einsum('bse,eh->bsh', behaviors, att_behav, precision=highest)
    pre_cand = jnp.einsum('bpe,eh->bph', candidates, att_cand, precision=highest) + att_bias
    activity = jax.nn.silu(pre_behav[:, None, :, :] + pre_cand[:, :, None, :])
    scores = jnp.einsum('bpsh,h->bps', activity, att_out, precision=highest) * live[:, None, :]
    pooled = jnp.einsum('bps,bse->bpe', scores, behaviors, precision=highest) / SEQ
    average = jnp.einsum('bs,bse->be', live, behaviors, precision=highest) / lens_block.astype(jnp.float32)[:, None]
    average = jnp.broadcast_to(average[:, None, :], pooled.shape)
    feature = jnp.concatenate([pooled, candidates, pooled * candidates, average], axis=-1)
    hidden = jax.nn.silu(jnp.einsum('bpf,fk->bpk', feature, dense_in, precision=highest) + dense_bias)
    logits = jnp.einsum('bpk,k->bp', hidden, dense_out, precision=highest)
    targets = labels_block.astype(jnp.float32)
    return jnp.sum(jax.nn.softplus(logits) - targets * logits)

def reference(behav_ids, lengths, cand_ids, labels, item_table, att_behav, att_cand, att_bias, att_out, dense_in, dense_bias, dense_out):
    params = (item_table, att_behav, att_cand, att_bias, att_out, dense_in, dense_bias, dense_out)
    ids_blocks = behav_ids.reshape(-1, USERS_DEV, SEQ)
    lens_blocks = lengths.reshape(-1, USERS_DEV)
    cands_blocks = cand_ids.reshape(-1, USERS_DEV, CANDS)
    labels_blocks = labels.reshape(-1, USERS_DEV, CANDS)

    def accumulate(carry, block):
        ids_block, lens_block, cands_block, labels_block = block

        def closed(*weights):
            return block_loss(*weights, ids_block, lens_block, cands_block, labels_block)
        value, pullback = jax.vjp(closed, *params)
        grads = pullback(jnp.ones_like(value))
        totals = jax.tree.map(lambda left, right: left + right, carry[1], grads)
        return ((carry[0] + value, totals), None)
    start = (jnp.zeros((), jnp.float32), tuple((jnp.zeros_like(weight) for weight in params)))
    (loss_total, grad_totals), _ = lax.scan(accumulate, start, (ids_blocks, lens_blocks, cands_blocks, labels_blocks))
    count = jnp.float32(USERS * CANDS)
    scaled = tuple((grad / count for grad in grad_totals))
    return (scaled[0], scaled[1], scaled[2], scaled[3], scaled[4], scaled[5], scaled[6], scaled[7], loss_total / count)
```

```python
import math

import jax
import jax.numpy as jnp
from jax import lax
from jax.experimental import pallas as pl
from jax.experimental.pallas import tpu as pltpu
from jax.sharding import PartitionSpec as P

AXES = ("batch", "rep")
F32 = jnp.float32
BF16 = jnp.bfloat16
NN = (((1,), (0,)), ((), ()))
NT = (((1,), (1,)), ((), ()))
TN = (((0,), (0,)), ((), ()))


def split(x):
    high = x.astype(BF16)
    return high, (x - high.astype(F32)).astype(BF16)


def dot(a, b, dims=NN):
    return lax.dot_general(a, b, dims, preferred_element_type=F32)


def dot3(a, b, dims=NN):
    (ah, al), (bh, bl) = a, b
    return dot(ah, bh, dims) + (dot(ah, bl, dims) + dot(al, bh, dims))


def local_kernel(
    place_ref, lens_ref, ids_ref, ids_col_ref, cand_col_ref, cand_row_ref, label_ref, table_ref,
    wb_ref, wc_ref, bias_ref, out_ref, din_ref, dbias_ref, dout_ref, order_ref,
    packed_ref,
    table_s, wbt_s, aob_s, prec_s, preb_s, b_s, scores_s, pooled_s, feat_s, dpool_s, davg_s,
    dprec_s, gtab_s, gwb_s, gao_s, dcand_s, full_s,
):
    users, seq = ids_ref.shape
    cats, width = table_ref.shape
    hid = wb_ref.shape[1]
    cands = cand_row_ref.shape[1] // users
    rows = users * cands
    lane = 128
    tiles = hid // 8

    th, tl = split(table_ref[...])
    table_s[:, :width] = th
    table_s[:, width:] = tl
    wbt = jnp.transpose(wb_ref[...])
    wct = jnp.transpose(wc_ref[...])
    wbt_half = split(0.5 * wbt)
    wct_half = split(0.5 * wct)
    bias_col = jnp.transpose(jnp.broadcast_to(bias_ref[...], (8, hid)))[:, :1]
    ao_col = jnp.transpose(jnp.broadcast_to(out_ref[...], (8, hid)))[:, :1]
    aob_s[...] = jnp.broadcast_to(ao_col, (hid, lane))
    wbt_s[...] = wbt

    ohc = (lax.broadcasted_iota(jnp.int32, (rows, cats), 1) == cand_col_ref[...]).astype(BF16)
    both = dot(ohc, table_s[...])
    cand = both[:, :width] + both[:, width:]
    cand_split = split(cand)
    prec_all = dot3(wct_half, cand_split, NT) + 0.5 * bias_col
    for u in range(users):
        prec_s[u] = prec_all[:, u * cands : (u + 1) * cands]
    feat_s[:, width : 2 * width] = cand

    ids_cols = ids_col_ref[...]
    iota_k = lax.broadcasted_iota(jnp.int32, (seq, cats), 1)
    iota_s = lax.broadcasted_iota(jnp.int32, (8, seq), 1)
    iota_u = lax.broadcasted_iota(jnp.int32, (seq, users), 1)
    group = 4

    def forward(u, carry):
        col = jnp.sum(jnp.where(iota_u == u, ids_cols, 0), axis=1, keepdims=True)
        oh = (iota_k == col).astype(BF16)
        both = dot(oh, table_s[...])
        b = both[:, :width] + both[:, width:]
        b_s[u] = b
        bsp = split(b)
        preb = dot3(wbt_half, bsp, NT)
        preb_s[u] = preb
        live = (iota_s < lens_ref[u]).astype(F32)
        prec = prec_s[u]
        for g0 in range(0, cands, group):
            accs = [jnp.zeros((8, seq), F32) for _ in range(group)]
            for t in range(tiles):
                sl = slice(8 * t, 8 * t + 8)
                pb = preb[sl]
                ao = aob_s[sl]
                ao = jnp.concatenate([ao, ao], axis=1)
                for j in range(group):
                    v = pb + prec[sl, g0 + j : g0 + j + 1]
                    act = v + v * jnp.tanh(v)
                    accs[j] = accs[j] + act * ao
            for j in range(group):
                sc = jnp.sum(accs[j], axis=0, keepdims=True) * live[:1]
                scores_s[u, g0 + j : g0 + j + 1, :] = sc
        scores_s[u, cands:, :] = live
        mix = dot3(split(scores_s[u]), bsp)
        base = pl.multiple_of(u * cands, cands)
        pooled_s[pl.ds(base, cands), :] = mix[:cands] * (1.0 / seq)
        avg = mix[cands : cands + 1] / lens_ref[u].astype(F32)
        feat_s[pl.ds(base, cands), 3 * width :] = jnp.broadcast_to(avg, (cands, width))
        return carry

    lax.fori_loop(0, users, forward, 0)

    pooled = pooled_s[...]
    cand = feat_s[:, width : 2 * width]
    feat_s[:, :width] = pooled
    feat_s[:, 2 * width : 3 * width] = pooled * cand
    fsp = split(feat_s[...])
    dsp = split(din_ref[...])
    z = 0.5 * (dot3(fsp, dsp) + dbias_ref[...])
    tz = jnp.tanh(z)
    q = 1.0 + tz
    hidden = z * q
    logit = jnp.sum(hidden * dout_ref[...], axis=1, keepdims=True)
    label = label_ref[...].astype(F32)
    loss_rows = jnp.maximum(logit, 0.0) + jnp.log1p(jnp.exp(-jnp.abs(logit))) - label * logit
    dlogit = 0.5 * (1.0 + jnp.tanh(0.5 * logit)) - label
    dz = (dlogit * dout_ref[...]) * (0.5 * (q + hidden * (1.0 - tz)))
    zsp = split(dz)
    gdin = dot3(fsp, zsp, TN)
    dfeat = dot3(zsp, dsp, NT)
    gdout = jnp.sum(dlogit * hidden, axis=0, keepdims=True)
    gdbias = jnp.sum(dz, axis=0, keepdims=True)
    loss = jnp.sum(loss_rows)
    dmix = dfeat[:, 2 * width : 3 * width]
    dpool_s[...] = (dfeat[:, :width] + dmix * cand) * (1.0 / seq)
    dcand_s[...] = dfeat[:, width : 2 * width] + dmix * pooled
    fin, fh = gdin.shape
    for j in range(fh // lane):
        full_s[cats + j * fin : cats + (j + 1) * fin, :] = gdin[:, j * lane : (j + 1) * lane]
    at = cats + fin * (fh // lane) + 2 * hid
    full_s[at:, :] = jnp.zeros((full_s.shape[0] - at, lane), F32)
    for j in range(fh // lane):
        full_s[at + 2 + j : at + 3 + j, :] = gdbias[:, j * lane : (j + 1) * lane]
        full_s[at + 2 + fh // lane + j : at + 3 + fh // lane + j, :] = gdout[:, j * lane : (j + 1) * lane]
    k = 2 + 2 * (fh // lane)
    full_s[at + k : at + k + 1, :] = jnp.full((1, lane), loss, F32)
    for u in range(users):
        part = jnp.sum(dfeat[u * cands : (u + 1) * cands, 3 * width :], axis=0, keepdims=True)
        davg_s[u : u + 1, :] = part / lens_ref[u].astype(F32)

    gtab_s[...] = jnp.zeros_like(gtab_s)
    gwb_s[...] = jnp.zeros_like(gwb_s)
    gao_s[...] = jnp.zeros_like(gao_s)
    iota_r = lax.broadcasted_iota(jnp.int32, (cats, seq), 0)
    first = lax.broadcasted_iota(jnp.int32, (8, width), 0) == 0

    def backward(u, carry):
        base = pl.multiple_of(u * cands, cands)
        dpool = dpool_s[pl.ds(base, cands), :]
        b = b_s[u]
        bsp = split(b)
        live = scores_s[u, cands : cands + 1, :]
        ds = dot3(split(dpool), bsp, NT) * live
        prec = prec_s[u]
        lane_i = lax.broadcasted_iota(jnp.int32, (8, lane), 1)
        dpre_tiles = []
        for t in range(tiles):
            sl = slice(8 * t, 8 * t + 8)
            pb = preb_s[u, sl, :]
            acc = jnp.zeros((8, seq), F32)
            gao = gao_s[sl, :]
            dpc = jnp.zeros((8, lane), F32)
            for p in range(cands):
                dsp_ = ds[p : p + 1, :]
                v = pb + prec[sl, p : p + 1]
                th_ = jnp.tanh(v)
                q_ = 1.0 + th_
                act = v * q_
                g = q_ + act * (1.0 - th_)
                gd = g * dsp_
                acc = acc + gd
                ad = act * dsp_
                gao = gao + (ad[:, :lane] + ad[:, lane:])
                red = jnp.sum(gd[:, :lane] + gd[:, lane:], axis=1, keepdims=True)
                dpc = jnp.where(lane_i == p, red, dpc)
            gao_s[sl, :] = gao
            half = 0.5 * aob_s[sl, :]
            dprec_s[u, sl, :] = (dpc * half)[:, :cands]
            dpre_tiles.append(acc * jnp.concatenate([half, half], axis=1))
        dpre = jnp.concatenate(dpre_tiles, axis=0)
        dpre_split = split(dpre)
        gwb_s[...] += dot3(dpre_split, bsp)
        davg = jnp.where(first, davg_s[pl.ds(u, 1), :], 0.0)
        left = split(jnp.concatenate([dpool, davg, wbt_s[...]], axis=0))
        right = split(jnp.concatenate([scores_s[u], dpre], axis=0))
        db = split(dot3(left, right, TN))
        ids_row = ids_ref[pl.ds(u, 1), :]
        oht = (iota_r == ids_row).astype(BF16)
        spread = dot(oht, jnp.concatenate(db, axis=0), NT)
        gtab_s[...] += spread[:, :width] + spread[:, width:]
        return carry

    lax.fori_loop(0, users, backward, 0)

    cand_split = split(feat_s[:, width : 2 * width])
    dprec = jnp.concatenate([dprec_s[u] for u in range(users)], axis=1)
    dprec_split = split(dprec)
    wct = split(jnp.transpose(wc_ref[...]))
    dcs = split(dcand_s[...] + dot3(dprec_split, wct, TN))
    ohr = (lax.broadcasted_iota(jnp.int32, (cats, rows), 0) == cand_row_ref[...]).astype(BF16)
    spread = dot(ohr, jnp.concatenate(dcs, axis=1))
    full_s[:cats, :] = gtab_s[...] + (spread[:, :width] + spread[:, width:])
    at = cats + fin * (fh // lane)
    full_s[at : at + hid, :] = gwb_s[...]
    full_s[at + hid : at + 2 * hid, :] = dot3(dprec_split, cand_split)
    at += 2 * hid
    ones_r = jnp.ones((8, rows), BF16)
    gbias = dot(ones_r, dprec_split[0], NT) + dot(ones_r, dprec_split[1], NT)
    full_s[at : at + 1, :hid] = gbias[:1]
    gao_split = split(gao_s[...])
    ones_l = jnp.ones((8, lane), BF16)
    gao_row = dot(ones_l, gao_split[0], NT) + dot(ones_l, gao_split[1], NT)
    full_s[at + 1 : at + 2, :hid] = gao_row[:1]

    chunks, chunk = packed_ref.shape[0], packed_ref.shape[1]

    def place(i, carry):
        src = pl.multiple_of((place_ref[0] ^ order_ref[i]) * chunk, 8)
        packed_ref[i] = full_s[pl.ds(src, chunk), :]
        return carry

    lax.fori_loop(0, chunks, place, 0)


def unpack_kernel(place_ref, order_ref, near_ref, far_ref, gtab_ref, gwb_ref, gwc_ref, gbias_ref, gout_ref, gdin_ref, gdb_ref, gdo_ref, loss_ref, full_s):
    half, chunk, lane = near_ref.shape

    def place(i, carry):
        dst = pl.multiple_of((place_ref[0] ^ order_ref[i]) * chunk, 8)
        full_s[pl.ds(dst, chunk), :] = near_ref[i]
        dst = pl.multiple_of((place_ref[0] ^ order_ref[half + i]) * chunk, 8)
        full_s[pl.ds(dst, chunk), :] = far_ref[i]
        return carry

    lax.fori_loop(0, half, place, 0)
    cats = gtab_ref.shape[0]
    fin, fh = gdin_ref.shape
    hid = gwb_ref.shape[1]
    at = 0
    gtab_ref[...] = full_s[:cats, :]
    at += cats
    for j in range(fh // lane):
        gdin_ref[:, j * lane : (j + 1) * lane] = full_s[at : at + fin, :]
        at += fin
    gwb_ref[...] = jnp.transpose(full_s[at : at + hid, :])
    at += hid
    gwc_ref[...] = jnp.transpose(full_s[at : at + hid, :])
    at += hid
    gbias_ref[...] = full_s[at : at + 1, :hid]
    gout_ref[...] = full_s[at + 1 : at + 2, :hid]
    for j in range(fh // lane):
        gdb_ref[:, j * lane : (j + 1) * lane] = full_s[at + 2 + j : at + 3 + j, :]
        gdo_ref[:, j * lane : (j + 1) * lane] = full_s[at + 2 + fh // lane + j : at + 3 + fh // lane + j, :]
    k = at + 2 + 2 * (fh // lane)
    loss_ref[...] = full_s[k : k + 1, :]


def combos(bits):
    found = [0]
    for bit in bits:
        found = found + [value | (1 << bit) for value in found]
    return found


def stages_of(batch, rep):
    low = rep.bit_length() - 1
    bits = list(range((batch * rep).bit_length() - 1))
    rest = [bit for bit in bits if bit != low]
    groups = [[low]]
    while rest:
        groups.append(rest[:2])
        rest = rest[2:]
    return groups


def body(behav_ids, lengths, cand_ids, labels, item_table, att_behav, att_cand, att_bias, att_out, dense_in, dense_bias, dense_out):
    batch = lax.axis_size("batch")
    rep = lax.axis_size("rep")
    devices = batch * rep
    users, seq = behav_ids.shape
    cands = cand_ids.shape[1]
    rows = users * cands
    cats, width = item_table.shape
    hid = att_behav.shape[1]
    fin, fh = dense_in.shape
    lane = 128
    tail = 3 + 2 * (fh // lane)
    need = cats + fin * (fh // lane) + 2 * hid + tail
    chunk = 8 * math.ceil(need / (8 * devices))
    groups = stages_of(batch, rep)
    order = [0]
    for group in groups:
        order = [a | b for a in order for b in combos(group)]
    order = jnp.array(order, jnp.int32)
    me = (lax.axis_index("batch") * rep + lax.axis_index("rep")).astype(jnp.int32)[None]

    smem = pl.BlockSpec(memory_space=pltpu.SMEM)
    vmem = pl.BlockSpec(memory_space=pltpu.VMEM)
    packed = pl.pallas_call(
        local_kernel,
        in_specs=[smem, smem] + [vmem] * 13 + [smem],
        out_specs=vmem,
        out_shape=jax.ShapeDtypeStruct((devices, chunk, lane), F32),
        scratch_shapes=[
            pltpu.VMEM((cats, 2 * width), BF16),
            pltpu.VMEM((hid, width), F32),
            pltpu.VMEM((hid, lane), F32),
            pltpu.VMEM((users, hid, cands), F32),
            pltpu.VMEM((users, hid, seq), F32),
            pltpu.VMEM((users, seq, width), F32),
            pltpu.VMEM((users, cands + 8, seq), F32),
            pltpu.VMEM((rows, width), F32),
            pltpu.VMEM((rows, fin), F32),
            pltpu.VMEM((rows, width), F32),
            pltpu.VMEM((users, width), F32),
            pltpu.VMEM((users, hid, cands), F32),
            pltpu.VMEM((cats, width), F32),
            pltpu.VMEM((hid, width), F32),
            pltpu.VMEM((hid, lane), F32),
            pltpu.VMEM((rows, width), F32),
            pltpu.VMEM((devices * chunk, lane), F32),
        ],
        name="local_step",
    )(
        me, lengths, behav_ids, behav_ids.T, cand_ids.reshape(rows, 1), cand_ids.reshape(1, rows),
        labels.reshape(rows, 1), item_table, att_behav, att_cand, att_bias[None], att_out[None],
        dense_in, dense_bias[None], dense_out[None], order,
    )

    x = packed
    for group in groups:
        steps = combos(group)
        x = x.reshape(len(steps), -1, lane)
        got = [
            lax.ppermute(x[i], AXES, [(d, d ^ step) for d in range(devices)])
            for i, step in enumerate(steps)
            if step
        ]
        x = x[0]
        for piece in got:
            x = x + piece
    x = x * (1.0 / (rows * devices))
    for group in reversed(groups[1:]):
        steps = combos(group)
        x = jnp.concatenate(
            [x] + [lax.ppermute(x, AXES, [(d, d ^ step) for d in range(devices)]) for step in steps if step],
            axis=0,
        )
    far = lax.ppermute(x, AXES, [(d, d ^ combos(groups[0])[1]) for d in range(devices)])
    half = devices // 2
    outs = pl.pallas_call(
        unpack_kernel,
        in_specs=[smem, smem, vmem, vmem],
        out_specs=[vmem] * 9,
        out_shape=[
            jax.ShapeDtypeStruct(shape, F32)
            for shape in (
                (cats, width), (width, hid), (width, hid), (1, hid), (1, hid), (fin, fh), (1, fh), (1, fh), (1, lane),
            )
        ],
        scratch_shapes=[pltpu.VMEM((devices * chunk, lane), F32)],
        name="unpack",
    )(me, order, x.reshape(half, chunk, lane), far.reshape(half, chunk, lane))
    gtab, gwb, gwc, gbias, gout, gdin, gdb, gdo, loss = outs
    return gtab, gwb, gwc, gbias[0], gout[0], gdin, gdb[0], gdo[0], loss[0, 0]


def solution(mesh):
    split_users = P(("batch", "rep"))
    placed = (split_users,) * 4 + (P(),) * 8
    return jax.shard_map(body, mesh=mesh, in_specs=placed, out_specs=(P(),) * 9, check_vma=False)
```

```python
import math

import jax
import jax.numpy as jnp
from jax import lax
from jax.experimental import pallas as pl
from jax.experimental.pallas import tpu as pltpu
from jax.sharding import PartitionSpec as P

AXES = ("batch", "rep")
F32 = jnp.float32
BF16 = jnp.bfloat16
NN = (((1,), (0,)), ((), ()))
NT = (((1,), (1,)), ((), ()))
TN = (((0,), (0,)), ((), ()))


def split(x):
    high = x.astype(BF16)
    return high, (x - high.astype(F32)).astype(BF16)


def dot(a, b, dims=NN):
    return lax.dot_general(a, b, dims, preferred_element_type=F32)


def dot3(a, b, dims=NN):
    (ah, al), (bh, bl) = a, b
    return dot(ah, bh, dims) + (dot(ah, bl, dims) + dot(al, bh, dims))


def local_kernel(
    place_ref, lens_ref, ids_ref, cand_ref, label_ref, table_ref, wbt_ref, wct_ref, bias_ref, out_ref,
    din_ref, dbias_ref, dout_ref, order_ref,
    near_ref, far_ref,
    table_s, aob_s, wside_s, prec_s, lin_s, idcol_s, preb_s, pbcur_s, pbnext_s, b_s, bnext_s, raw_s, scst_s,
    feat_s, dpst_s, ds_s, dprec_s, dcur_s, dprev_s, gtab_s, gwb_s, gao_s, dcand_s, full_s,
):
    users, seq = ids_ref.shape
    cats, width = table_ref.shape
    hid = wbt_ref.shape[0]
    cands = cand_ref.shape[1]
    rows = users * cands
    lane = 128
    tiles = hid // 8
    pad = 2 * cands
    one, zero = BF16(1), BF16(0)

    th, tl = split(table_ref[...])
    table_s[:, :width] = th
    table_s[:, width:] = tl
    wbh, wbl = split(0.5 * wbt_ref[...])
    wbhh = jnp.concatenate([wbh, wbh], axis=1)
    wch, wcl = split(0.5 * wct_ref[...])
    wh, wl = split(jnp.transpose(wbt_ref[...]))
    wside_s[:, :hid] = wh
    wside_s[:, hid : 2 * hid] = wh
    wside_s[:, 2 * hid :] = wl
    bias_col = jnp.transpose(jnp.broadcast_to(bias_ref[...], (8, hid)))[:, :1]
    ao_col = jnp.transpose(jnp.broadcast_to(out_ref[...], (8, hid)))[:, :1]
    aob_s[...] = jnp.broadcast_to(ao_col, (hid, lane))

    idcol_s[...] = jnp.transpose(ids_ref[...].astype(F32))
    cand_t = jnp.transpose(jnp.concatenate([cand_ref[...].astype(F32)] * (lane // cands), axis=1))
    cand_col = jnp.concatenate([cand_t[:cands, u : u + 1] for u in range(users)], axis=0)
    label_t = jnp.transpose(jnp.concatenate([label_ref[...].astype(F32)] * (lane // cands), axis=1))
    label = jnp.concatenate([label_t[:cands, u : u + 1] for u in range(users)], axis=0)

    def onehot(col, n):
        wide = jnp.broadcast_to(col, (n, lane)).astype(jnp.int32).astype(jnp.int16)
        iota = lax.broadcasted_iota(jnp.int16, (n, lane), 1)
        return jnp.concatenate(
            [jnp.where(wide - jnp.int16(lane * k) == iota, one, zero) for k in range(cats // lane)], axis=1
        )

    pair = dot(onehot(cand_col, rows), table_s[...])
    cand = pair[:, :width] + pair[:, width:]
    cpair = pair.astype(BF16)
    prec_all = (
        dot(jnp.concatenate([wch, wch], axis=1), cpair, NT) + dot(wcl, cpair[:, :width], NT) + 0.5 * bias_col
    )
    for u in range(users):
        prec_s[u] = prec_all[:, u * cands : (u + 1) * cands]
    lin_row = jnp.broadcast_to(jnp.sum(prec_all * ao_col, axis=0, keepdims=True), (lane, rows))
    lin_s[...] = jnp.transpose(lin_row)
    feat_s[:, width : 2 * width] = cand

    iota_u = lax.broadcasted_iota(jnp.int32, (lane, users), 1)
    iota_s = lax.broadcasted_iota(jnp.int32, (cands, seq), 1)
    group = 4

    def fetch(u, at):
        cols = idcol_s[at : at + lane, :]
        col = jnp.sum(jnp.where(iota_u == u, cols, 0.0), axis=1, keepdims=True)
        bnext_s[at : at + lane, :] = dot(onehot(col, lane), table_s[...]).astype(BF16)

    def project():
        b = bnext_s[...]
        pbnext_s[...] = dot(wbhh, b, NT) + dot(wbl, b[:, :width], NT)

    for at in range(0, seq, lane):
        fetch(0, at)
    project()

    def forward(u, carry):
        b_s[u] = bnext_s[...]
        pb_all = pbnext_s[...]
        preb_s[u] = pb_all
        pbcur_s[...] = pb_all
        following = jnp.minimum(u + 1, users - 1)
        lin = jnp.zeros((8, seq), F32)
        for g0 in range(0, cands, group):
            if g0 // group < seq // lane:
                fetch(following, g0 // group * lane)
            elif g0 // group == seq // lane:
                project()
            accs = [jnp.zeros((8, seq), F32) for _ in range(group)]
            for t in range(tiles):
                sl = slice(8 * t, 8 * t + 8)
                pb = pbcur_s[sl, :]
                ao = aob_s[sl, :]
                ao = jnp.concatenate([ao] * (seq // lane), axis=1)
                if g0 == 0:
                    lin = lin + ao * pb
                for j in range(group):
                    v = pb + prec_s[u, sl, g0 + j : g0 + j + 1]
                    accs[j] = accs[j] + (ao * v) * jnp.tanh(v)
            for j in range(group):
                raw_s[g0 + j : g0 + j + 1, :] = jnp.sum(accs[j] + lin, axis=0, keepdims=True)
        live = (iota_s < lens_ref[u]).astype(F32)
        base = pl.multiple_of(u * cands, cands)
        lin_c = lin_s[pl.ds(base, cands), :]
        sc = (raw_s[...] + jnp.concatenate([lin_c] * (seq // lane), axis=1)) * live
        sh, sl_ = split(sc)
        lh = live.astype(BF16)
        scst_s[u, :cands, :] = sh
        scst_s[u, cands:pad, :] = lh
        scst_s[u, pad : pad + cands, :] = sl_
        scst_s[u, pad + cands : 2 * pad, :] = jnp.zeros((cands, seq), BF16)
        scst_s[u, 2 * pad : 2 * pad + cands, :] = sh
        scst_s[u, 2 * pad + cands :, :] = lh
        return carry

    lax.fori_loop(0, users, forward, 0)

    for u in range(users):
        b = b_s[u]
        wide = dot(scst_s[u, :pad, :], b)
        mix = wide[:, :width] + wide[:, width:] + dot(scst_s[u, pad : 2 * pad, :], b[:, :width])
        feat_s[u * cands : (u + 1) * cands, :width] = mix[:cands] * (1.0 / seq)
        avg = mix[cands : cands + 1] / lens_ref[u].astype(F32)
        feat_s[u * cands : (u + 1) * cands, 3 * width :] = jnp.broadcast_to(avg, (cands, width))

    pooled = feat_s[:, :width]
    cand = feat_s[:, width : 2 * width]
    feat_s[:, 2 * width : 3 * width] = pooled * cand
    fsp = split(feat_s[...])
    dsp = split(din_ref[...])
    z = 0.5 * (dot3(fsp, dsp) + dbias_ref[...])
    tz = jnp.tanh(z)
    q = 1.0 + tz
    hidden = z * q
    logit = jnp.sum(hidden * dout_ref[...], axis=1, keepdims=True)
    loss_rows = jnp.maximum(logit, 0.0) + jnp.log1p(jnp.exp(-jnp.abs(logit))) - label * logit
    dlogit = 0.5 * (1.0 + jnp.tanh(0.5 * logit)) - label
    dz = (dlogit * dout_ref[...]) * (0.5 * (q + hidden * (1.0 - tz)))
    zsp = split(dz)
    dfeat = dot3(zsp, dsp, NT)
    gdin = dot3(fsp, zsp, TN)
    gdout = jnp.sum(dlogit * hidden, axis=0, keepdims=True)
    gdbias = jnp.sum(dz, axis=0, keepdims=True)
    loss = jnp.sum(loss_rows)
    dmix = dfeat[:, 2 * width : 3 * width]
    dpool = (dfeat[:, :width] + dmix * cand) * (1.0 / seq)
    dcand_s[...] = dfeat[:, width : 2 * width] + dmix * pooled
    fin, fh = gdin.shape
    for j in range(fh // lane):
        full_s[cats + j * fin : cats + (j + 1) * fin, :] = gdin[:, j * lane : (j + 1) * lane]
    at = cats + fin * (fh // lane) + 2 * hid
    full_s[at:, :] = jnp.zeros((full_s.shape[0] - at, lane), F32)
    for j in range(fh // lane):
        full_s[at + 2 + j : at + 3 + j, :] = gdbias[:, j * lane : (j + 1) * lane]
        full_s[at + 2 + fh // lane + j : at + 3 + fh // lane + j, :] = gdout[:, j * lane : (j + 1) * lane]
    k = 2 + 2 * (fh // lane)
    full_s[at + k : at + k + 1, :] = jnp.full((1, lane), loss, F32)

    first = lax.broadcasted_iota(jnp.int32, (cands, width), 0) == 0
    for u in range(users):
        part = jnp.sum(dfeat[u * cands : (u + 1) * cands, 3 * width :], axis=0, keepdims=True)
        davg = jnp.where(first, part / lens_ref[u].astype(F32), 0.0)
        dh, dl = split(jnp.concatenate([dpool[u * cands : (u + 1) * cands], davg], axis=0))
        dpst_s[u, :pad, :] = dh
        dpst_s[u, pad : 2 * pad, :] = dh
        dpst_s[u, 2 * pad :, :] = dl
        b = b_s[u]
        live = (iota_s < lens_ref[u]).astype(F32)
        grad = dot(jnp.concatenate([dh[:cands], dh[:cands]], axis=1), b, NT) + dot(dl[:cands], b[:, :width], NT)
        ds_s[u] = grad * live

    gtab_s[...] = jnp.zeros_like(gtab_s)
    gwb_s[...] = jnp.zeros_like(gwb_s)
    gao_s[...] = jnp.zeros_like(gao_s)
    dprev_s[...] = jnp.zeros_like(dprev_s)
    lane_i = lax.broadcasted_iota(jnp.int32, (8, lane), 1)
    block = cats // 4

    def finish_weights(u, keep):
        ph, pl_ = split(dprev_s[...])
        b = b_s[u]
        wide = dot(ph, b)
        gwb_s[...] += wide[:, :width] + wide[:, width:] + dot(pl_, b[:, :width])
        db = dot(wside_s[...], jnp.concatenate([ph, pl_, ph], axis=0))
        db = db + dot(dpst_s[u] * keep, scst_s[u], TN)
        return jnp.concatenate(split(db), axis=0)

    def finish_rows(u, db, part):
        row = jnp.broadcast_to(ids_ref[pl.ds(u, 1), :], (16, seq)).astype(jnp.int16)
        iota = lax.broadcasted_iota(jnp.int16, (16, seq), 0)
        start = part * block
        hot = jnp.concatenate(
            [jnp.where(row - jnp.int16(start + k) == iota, one, zero) for k in range(0, block, 16)], axis=0
        )
        spread = dot(hot, db, NT)
        gtab_s[start : start + block, :] += spread[:, :width] + spread[:, width:]

    def backward(u, carry):
        prev = jnp.maximum(u - 1, 0)
        keep = (u > 0).astype(F32).astype(BF16)
        db = None
        for t in range(tiles):
            if t == 0:
                db = finish_weights(prev, keep)
            if t >= 2 and t % 2 == 0:
                finish_rows(prev, db, t // 2 - 1)
            sl = slice(8 * t, 8 * t + 8)
            pb = preb_s[u, sl, :]
            acc = jnp.zeros((8, seq), F32)
            gao = gao_s[sl, :]
            dpc = jnp.zeros((8, lane), F32)
            for p in range(cands):
                grad = ds_s[u, p : p + 1, :]
                v = pb + prec_s[u, sl, p : p + 1]
                th_ = jnp.tanh(v)
                q_ = 1.0 + th_
                act = v * q_
                gd = (q_ + act * (1.0 - th_)) * grad
                acc = acc + gd
                ad = act * grad
                gao = gao + (ad[:, :lane] + ad[:, lane:])
                red = jnp.sum(gd[:, :lane] + gd[:, lane:], axis=1, keepdims=True)
                dpc = jnp.where(lane_i == p, red, dpc)
            gao_s[sl, :] = gao
            half = 0.5 * aob_s[sl, :]
            dprec_s[u, sl, :] = (dpc * half)[:, :cands]
            dcur_s[sl, :] = acc * jnp.concatenate([half] * (seq // lane), axis=1)
        dprev_s[...] = dcur_s[...]
        return carry

    lax.fori_loop(0, users, backward, 0)
    db = finish_weights(users - 1, one)
    for part in range(4):
        finish_rows(users - 1, db, part)

    ch, cl = split(feat_s[:, width : 2 * width])
    dprec = jnp.concatenate([dprec_s[u] for u in range(users)], axis=1)
    dph, dpl = split(dprec)
    wct = split(wct_ref[...])
    dcs = split(dcand_s[...] + dot3((dph, dpl), wct, TN))
    cand_t = jnp.transpose(jnp.concatenate([cand_ref[...].astype(F32)] * (lane // cands), axis=1))
    cand_col = jnp.concatenate([cand_t[:cands, u : u + 1] for u in range(users)], axis=0)
    cand_row = jnp.transpose(jnp.broadcast_to(cand_col, (rows, lane)))[:16].astype(jnp.int32).astype(jnp.int16)
    iota = lax.broadcasted_iota(jnp.int16, (16, rows), 0)
    hot = jnp.concatenate(
        [jnp.where(cand_row - jnp.int16(k) == iota, one, zero) for k in range(0, cats, 16)], axis=0
    )
    spread = dot(hot, jnp.concatenate(dcs, axis=1))
    full_s[:cats, :] = gtab_s[...] + (spread[:, :width] + spread[:, width:])
    at = cats + fin * (fh // lane)
    full_s[at : at + hid, :] = gwb_s[...]
    full_s[at + hid : at + 2 * hid, :] = dot3((dph, dpl), (ch, cl))
    at += 2 * hid
    ones_r = jnp.ones((8, rows), BF16)
    gbias = dot(ones_r, dph, NT) + dot(ones_r, dpl, NT)
    full_s[at : at + 1, :hid] = gbias[:1]
    gao_split = split(gao_s[...])
    ones_l = jnp.ones((8, lane), BF16)
    gao_row = dot(ones_l, gao_split[0], NT) + dot(ones_l, gao_split[1], NT)
    full_s[at + 1 : at + 2, :hid] = gao_row[:1]

    half, chunk = near_ref.shape[0], near_ref.shape[1]

    def place(i, carry):
        src = pl.multiple_of((place_ref[0] ^ order_ref[i]) * chunk, 8)
        near_ref[i] = full_s[pl.ds(src, chunk), :]
        src = pl.multiple_of((place_ref[0] ^ order_ref[half + i]) * chunk, 8)
        far_ref[i] = full_s[pl.ds(src, chunk), :]
        return carry

    lax.fori_loop(0, half, place, 0)


def unpack_kernel(place_ref, order_ref, near_ref, far_ref, gtab_ref, gwb_ref, gwc_ref, gbias_ref, gout_ref, gdin_ref, gdb_ref, gdo_ref, loss_ref, full_s):
    half, chunk, lane = near_ref.shape

    def place(i, carry):
        dst = pl.multiple_of((place_ref[0] ^ order_ref[i]) * chunk, 8)
        full_s[pl.ds(dst, chunk), :] = near_ref[i]
        dst = pl.multiple_of((place_ref[0] ^ order_ref[half + i]) * chunk, 8)
        full_s[pl.ds(dst, chunk), :] = far_ref[i]
        return carry

    lax.fori_loop(0, half, place, 0)
    cats = gtab_ref.shape[0]
    fin, fh = gdin_ref.shape
    hid = gwb_ref.shape[0]
    at = 0
    gtab_ref[...] = full_s[:cats, :]
    at += cats
    for j in range(fh // lane):
        gdin_ref[:, j * lane : (j + 1) * lane] = full_s[at : at + fin, :]
        at += fin
    gwb_ref[...] = full_s[at : at + hid, :]
    at += hid
    gwc_ref[...] = full_s[at : at + hid, :]
    at += hid
    gbias_ref[...] = full_s[at : at + 1, :hid]
    gout_ref[...] = full_s[at + 1 : at + 2, :hid]
    for j in range(fh // lane):
        gdb_ref[:, j * lane : (j + 1) * lane] = full_s[at + 2 + j : at + 3 + j, :]
        gdo_ref[:, j * lane : (j + 1) * lane] = full_s[at + 2 + fh // lane + j : at + 3 + fh // lane + j, :]
    k = at + 2 + 2 * (fh // lane)
    loss_ref[...] = full_s[k : k + 1, :]


def combos(bits):
    found = [0]
    for bit in bits:
        found = found + [value | (1 << bit) for value in found]
    return found


def stages_of(batch, rep):
    low = rep.bit_length() - 1
    bits = list(range((batch * rep).bit_length() - 1))
    rest = [bit for bit in bits if bit != low]
    groups = [[low]]
    while rest:
        groups.append(rest[:2])
        rest = rest[2:]
    return groups


def body(behav_ids, lengths, cand_ids, labels, item_table, att_behav, att_cand, att_bias, att_out, dense_in, dense_bias, dense_out):
    batch = lax.axis_size("batch")
    rep = lax.axis_size("rep")
    devices = batch * rep
    users, seq = behav_ids.shape
    cands = cand_ids.shape[1]
    rows = users * cands
    cats, width = item_table.shape
    hid = att_behav.shape[1]
    fin, fh = dense_in.shape
    lane = 128
    tail = 3 + 2 * (fh // lane)
    need = cats + fin * (fh // lane) + 2 * hid + tail
    chunk = 8 * math.ceil(need / (8 * devices))
    groups = stages_of(batch, rep)
    order = [0]
    for group in groups:
        order = [a | b for a in order for b in combos(group)]
    order = jnp.array(order, jnp.int32)
    me = (lax.axis_index("batch") * rep + lax.axis_index("rep")).astype(jnp.int32)[None]

    smem = pl.BlockSpec(memory_space=pltpu.SMEM)
    vmem = pl.BlockSpec(memory_space=pltpu.VMEM)
    half = devices // 2
    near, far = pl.pallas_call(
        local_kernel,
        in_specs=[smem, smem] + [vmem] * 11 + [smem],
        out_specs=[vmem, vmem],
        out_shape=[jax.ShapeDtypeStruct((half, chunk, lane), F32)] * 2,
        scratch_shapes=[
            pltpu.VMEM((cats, 2 * width), BF16),
            pltpu.VMEM((hid, lane), F32),
            pltpu.VMEM((width, 3 * hid), BF16),
            pltpu.VMEM((users, hid, cands), F32),
            pltpu.VMEM((rows, lane), F32),
            pltpu.VMEM((seq, users), F32),
            pltpu.VMEM((users, hid, seq), F32),
            pltpu.VMEM((hid, seq), F32),
            pltpu.VMEM((hid, seq), F32),
            pltpu.VMEM((users, seq, 2 * width), BF16),
            pltpu.VMEM((seq, 2 * width), BF16),
            pltpu.VMEM((cands, seq), F32),
            pltpu.VMEM((users, 6 * cands, seq), BF16),
            pltpu.VMEM((rows, fin), F32),
            pltpu.VMEM((users, 6 * cands, width), BF16),
            pltpu.VMEM((users, cands, seq), F32),
            pltpu.VMEM((users, hid, cands), F32),
            pltpu.VMEM((hid, seq), F32),
            pltpu.VMEM((hid, seq), F32),
            pltpu.VMEM((cats, width), F32),
            pltpu.VMEM((hid, width), F32),
            pltpu.VMEM((hid, lane), F32),
            pltpu.VMEM((rows, width), F32),
            pltpu.VMEM((devices * chunk, lane), F32),
        ],
        name="local_step",
    )(
        me, lengths, behav_ids, cand_ids, labels, item_table, att_behav.T, att_cand.T, att_bias[None],
        att_out[None], dense_in, dense_bias[None], dense_out[None], order,
    )

    pair = [(d, d ^ combos(groups[0])[1]) for d in range(devices)]
    x = near.reshape(half * chunk, lane) + lax.ppermute(far.reshape(half * chunk, lane), AXES, pair)
    for group in groups[1:]:
        steps = combos(group)
        x = x.reshape(len(steps), -1, lane)
        got = [
            lax.ppermute(x[i], AXES, [(d, d ^ step) for d in range(devices)])
            for i, step in enumerate(steps)
            if step
        ]
        x = x[0]
        for piece in got:
            x = x + piece
    x = x * (1.0 / (rows * devices))
    for group in reversed(groups[1:]):
        steps = combos(group)
        x = jnp.concatenate(
            [x] + [lax.ppermute(x, AXES, [(d, d ^ step) for d in range(devices)]) for step in steps if step],
            axis=0,
        )
    far = lax.ppermute(x, AXES, pair)
    outs = pl.pallas_call(
        unpack_kernel,
        in_specs=[smem, smem, vmem, vmem],
        out_specs=[vmem] * 9,
        out_shape=[
            jax.ShapeDtypeStruct(shape, F32)
            for shape in (
                (cats, width), (hid, width), (hid, width), (1, hid), (1, hid), (fin, fh), (1, fh), (1, fh), (1, lane),
            )
        ],
        scratch_shapes=[pltpu.VMEM((devices * chunk, lane), F32)],
        name="unpack",
    )(me, order, x.reshape(half, chunk, lane), far.reshape(half, chunk, lane))
    gtab, gwb, gwc, gbias, gout, gdin, gdb, gdo, loss = outs
    return gtab, gwb.T, gwc.T, gbias[0], gout[0], gdin, gdb[0], gdo[0], loss[0, 0]


def solution(mesh):
    split_users = P(("batch", "rep"))
    placed = (split_users,) * 4 + (P(),) * 8
    return jax.shard_map(body, mesh=mesh, in_specs=placed, out_specs=(P(),) * 9, check_vma=False)
```

```python
import math

import jax
import jax.numpy as jnp
from jax import lax
from jax.experimental import pallas as pl
from jax.experimental.pallas import tpu as pltpu
from jax.sharding import PartitionSpec as P

AXES = ("batch", "rep")
F32 = jnp.float32
BF16 = jnp.bfloat16
NN = (((1,), (0,)), ((), ()))
NT = (((1,), (1,)), ((), ()))
TN = (((0,), (0,)), ((), ()))


def split(x):
    high = x.astype(BF16)
    return high, (x - high.astype(F32)).astype(BF16)


def dot(a, b, dims=NN):
    return lax.dot_general(a, b, dims, preferred_element_type=F32)


def dot3(a, b, dims=NN):
    (ah, al), (bh, bl) = a, b
    return dot(ah, bh, dims) + (dot(ah, bl, dims) + dot(al, bh, dims))


def local_kernel(
    place_ref, lens_ref, ids_ref, cand_ref, label_ref, table_ref, wbt_ref, wct_ref, bias_ref, out_ref,
    din_ref, dbias_ref, dout_ref,
    near_ref, far_ref,
    table_s, aob_s, wside_s, prec_s, lin_s, idcol_s, preb_s, pbcur_s, pbnext_s, b_s, bnext_s, raw_s, scst_s,
    feat_s, dpst_s, ds_s, dprec_s, dcur_s, dprev_s, gtab_s, gwb_s, gao_s, dcand_s, full_s,
):
    users, seq = ids_ref.shape
    cats, width = table_ref.shape
    hid = wbt_ref.shape[0]
    cands = cand_ref.shape[1]
    rows = users * cands
    lane = 128
    tiles = hid // 8
    pad = 2 * cands
    one, zero = BF16(1), BF16(0)

    th, tl = split(table_ref[...])
    table_s[:, :width] = th
    table_s[:, width:] = tl
    wbh, wbl = split(0.5 * wbt_ref[...])
    wbhh = jnp.concatenate([wbh, wbh], axis=1)
    wch, wcl = split(0.5 * wct_ref[...])
    wh, wl = split(jnp.transpose(wbt_ref[...]))
    wside_s[:, :hid] = wh
    wside_s[:, hid : 2 * hid] = wh
    wside_s[:, 2 * hid :] = wl
    bias_col = jnp.transpose(jnp.broadcast_to(bias_ref[...], (8, hid)))[:, :1]
    ao_col = jnp.transpose(jnp.broadcast_to(out_ref[...], (8, hid)))[:, :1]
    aob_s[...] = jnp.broadcast_to(ao_col, (hid, lane))

    idcol_s[...] = jnp.transpose(ids_ref[...].astype(F32))
    cand_t = jnp.transpose(jnp.concatenate([cand_ref[...].astype(F32)] * (lane // cands), axis=1))
    cand_col = jnp.concatenate([cand_t[:cands, u : u + 1] for u in range(users)], axis=0)
    label_t = jnp.transpose(jnp.concatenate([label_ref[...].astype(F32)] * (lane // cands), axis=1))
    label = jnp.concatenate([label_t[:cands, u : u + 1] for u in range(users)], axis=0)

    def onehot(col, n):
        wide = jnp.broadcast_to(col, (n, lane)).astype(jnp.int32).astype(jnp.int16)
        iota = lax.broadcasted_iota(jnp.int16, (n, lane), 1)
        return jnp.concatenate(
            [jnp.where(wide - jnp.int16(lane * k) == iota, one, zero) for k in range(cats // lane)], axis=1
        )

    pair = dot(onehot(cand_col, rows), table_s[...])
    cand = pair[:, :width] + pair[:, width:]
    cpair = pair.astype(BF16)
    prec_all = (
        dot(jnp.concatenate([wch, wch], axis=1), cpair, NT) + dot(wcl, cpair[:, :width], NT) + 0.5 * bias_col
    )
    for u in range(users):
        prec_s[u] = prec_all[:, u * cands : (u + 1) * cands]
    lin_row = jnp.broadcast_to(jnp.sum(prec_all * ao_col, axis=0, keepdims=True), (lane, rows))
    lin_s[...] = jnp.transpose(lin_row)
    feat_s[:, width : 2 * width] = cand

    iota_u = lax.broadcasted_iota(jnp.int32, (lane, users), 1)
    iota_s = lax.broadcasted_iota(jnp.int32, (cands, seq), 1)
    group = 4

    def fetch(u, at):
        cols = idcol_s[at : at + lane, :]
        col = jnp.sum(jnp.where(iota_u == u, cols, 0.0), axis=1, keepdims=True)
        bnext_s[at : at + lane, :] = dot(onehot(col, lane), table_s[...]).astype(BF16)

    def project():
        b = bnext_s[...]
        pbnext_s[...] = dot(wbhh, b, NT) + dot(wbl, b[:, :width], NT)

    for at in range(0, seq, lane):
        fetch(0, at)
    project()

    def forward(u, carry):
        b_s[u] = bnext_s[...]
        pb_all = pbnext_s[...]
        preb_s[u] = pb_all
        pbcur_s[...] = pb_all
        following = jnp.minimum(u + 1, users - 1)
        lin = jnp.zeros((8, seq), F32)
        for g0 in range(0, cands, group):
            if g0 // group < seq // lane:
                fetch(following, g0 // group * lane)
            elif g0 // group == seq // lane:
                project()
            accs = [jnp.zeros((8, seq), F32) for _ in range(group)]
            for t in range(tiles):
                sl = slice(8 * t, 8 * t + 8)
                pb = pbcur_s[sl, :]
                ao = aob_s[sl, :]
                ao = jnp.concatenate([ao] * (seq // lane), axis=1)
                if g0 == 0:
                    lin = lin + ao * pb
                for j in range(group):
                    v = pb + prec_s[u, sl, g0 + j : g0 + j + 1]
                    accs[j] = accs[j] + (ao * v) * jnp.tanh(v)
            for j in range(group):
                raw_s[g0 + j : g0 + j + 1, :] = jnp.sum(accs[j] + lin, axis=0, keepdims=True)
        live = (iota_s < lens_ref[u]).astype(F32)
        base = pl.multiple_of(u * cands, cands)
        lin_c = lin_s[pl.ds(base, cands), :]
        sc = (raw_s[...] + jnp.concatenate([lin_c] * (seq // lane), axis=1)) * live
        sh, sl_ = split(sc)
        lh = live.astype(BF16)
        scst_s[u, :cands, :] = sh
        scst_s[u, cands:pad, :] = lh
        scst_s[u, pad : pad + cands, :] = sl_
        scst_s[u, pad + cands : 2 * pad, :] = jnp.zeros((cands, seq), BF16)
        scst_s[u, 2 * pad : 2 * pad + cands, :] = sh
        scst_s[u, 2 * pad + cands :, :] = lh
        return carry

    lax.fori_loop(0, users, forward, 0)

    for u in range(users):
        b = b_s[u]
        wide = dot(scst_s[u, :pad, :], b)
        mix = wide[:, :width] + wide[:, width:] + dot(scst_s[u, pad : 2 * pad, :], b[:, :width])
        feat_s[u * cands : (u + 1) * cands, :width] = mix[:cands] * (1.0 / seq)
        avg = mix[cands : cands + 1] / lens_ref[u].astype(F32)
        feat_s[u * cands : (u + 1) * cands, 3 * width :] = jnp.broadcast_to(avg, (cands, width))

    pooled = feat_s[:, :width]
    cand = feat_s[:, width : 2 * width]
    feat_s[:, 2 * width : 3 * width] = pooled * cand
    fsp = split(feat_s[...])
    dsp = split(din_ref[...])
    z = 0.5 * (dot3(fsp, dsp) + dbias_ref[...])
    tz = jnp.tanh(z)
    q = 1.0 + tz
    hidden = z * q
    logit = jnp.sum(hidden * dout_ref[...], axis=1, keepdims=True)
    loss_rows = jnp.maximum(logit, 0.0) + jnp.log1p(jnp.exp(-jnp.abs(logit))) - label * logit
    dlogit = 0.5 * (1.0 + jnp.tanh(0.5 * logit)) - label
    dz = (dlogit * dout_ref[...]) * (0.5 * (q + hidden * (1.0 - tz)))
    zsp = split(dz)
    dfeat = dot3(zsp, dsp, NT)
    gdin = dot3(fsp, zsp, TN)
    gdout = jnp.sum(dlogit * hidden, axis=0, keepdims=True)
    gdbias = jnp.sum(dz, axis=0, keepdims=True)
    loss = jnp.sum(loss_rows)
    dmix = dfeat[:, 2 * width : 3 * width]
    dpool = (dfeat[:, :width] + dmix * cand) * (1.0 / seq)
    dcand_s[...] = dfeat[:, width : 2 * width] + dmix * pooled
    fin, fh = gdin.shape
    for j in range(fh // lane):
        full_s[cats + j * fin : cats + (j + 1) * fin, :] = gdin[:, j * lane : (j + 1) * lane]
    at = cats + fin * (fh // lane) + 2 * hid
    full_s[at:, :] = jnp.zeros((full_s.shape[0] - at, lane), F32)
    for j in range(fh // lane):
        full_s[at + 2 + j : at + 3 + j, :] = gdbias[:, j * lane : (j + 1) * lane]
        full_s[at + 2 + fh // lane + j : at + 3 + fh // lane + j, :] = gdout[:, j * lane : (j + 1) * lane]
    k = 2 + 2 * (fh // lane)
    full_s[at + k : at + k + 1, :] = jnp.full((1, lane), loss, F32)

    first = lax.broadcasted_iota(jnp.int32, (cands, width), 0) == 0
    for u in range(users):
        part = jnp.sum(dfeat[u * cands : (u + 1) * cands, 3 * width :], axis=0, keepdims=True)
        davg = jnp.where(first, part / lens_ref[u].astype(F32), 0.0)
        dh, dl = split(jnp.concatenate([dpool[u * cands : (u + 1) * cands], davg], axis=0))
        dpst_s[u, :pad, :] = dh
        dpst_s[u, pad : 2 * pad, :] = dh
        dpst_s[u, 2 * pad :, :] = dl
        b = b_s[u]
        live = (iota_s < lens_ref[u]).astype(F32)
        grad = dot(jnp.concatenate([dh[:cands], dh[:cands]], axis=1), b, NT) + dot(dl[:cands], b[:, :width], NT)
        ds_s[u] = grad * live

    gtab_s[...] = jnp.zeros_like(gtab_s)
    gwb_s[...] = jnp.zeros_like(gwb_s)
    gao_s[...] = jnp.zeros_like(gao_s)
    dprev_s[...] = jnp.zeros_like(dprev_s)
    lane_i = lax.broadcasted_iota(jnp.int32, (8, lane), 1)
    block = cats // 4

    def finish_weights(u, keep):
        ph, pl_ = split(dprev_s[...])
        b = b_s[u]
        wide = dot(ph, b)
        gwb_s[...] += wide[:, :width] + wide[:, width:] + dot(pl_, b[:, :width])
        db = dot(wside_s[...], jnp.concatenate([ph, pl_, ph], axis=0))
        db = db + dot(dpst_s[u] * keep, scst_s[u], TN)
        return jnp.concatenate(split(db), axis=0)

    def finish_rows(u, db, part):
        row = jnp.broadcast_to(ids_ref[pl.ds(u, 1), :], (16, seq)).astype(jnp.int16)
        iota = lax.broadcasted_iota(jnp.int16, (16, seq), 0)
        start = part * block
        hot = jnp.concatenate(
            [jnp.where(row - jnp.int16(start + k) == iota, one, zero) for k in range(0, block, 16)], axis=0
        )
        spread = dot(hot, db, NT)
        gtab_s[start : start + block, :] += spread[:, :width] + spread[:, width:]

    def backward(u, carry):
        prev = jnp.maximum(u - 1, 0)
        keep = (u > 0).astype(F32).astype(BF16)
        db = None
        for t in range(tiles):
            if t == 0:
                db = finish_weights(prev, keep)
            if t >= 2 and t % 2 == 0:
                finish_rows(prev, db, t // 2 - 1)
            sl = slice(8 * t, 8 * t + 8)
            pb = preb_s[u, sl, :]
            acc = jnp.zeros((8, seq), F32)
            gao = gao_s[sl, :]
            dpc = jnp.zeros((8, lane), F32)
            for p in range(cands):
                grad = ds_s[u, p : p + 1, :]
                v = pb + prec_s[u, sl, p : p + 1]
                th_ = jnp.tanh(v)
                q_ = 1.0 + th_
                act = v * q_
                gd = (q_ + act * (1.0 - th_)) * grad
                acc = acc + gd
                ad = act * grad
                gao = gao + (ad[:, :lane] + ad[:, lane:])
                red = jnp.sum(gd[:, :lane] + gd[:, lane:], axis=1, keepdims=True)
                dpc = jnp.where(lane_i == p, red, dpc)
            gao_s[sl, :] = gao
            half = 0.5 * aob_s[sl, :]
            dprec_s[u, sl, :] = (dpc * half)[:, :cands]
            dcur_s[sl, :] = acc * jnp.concatenate([half] * (seq // lane), axis=1)
        dprev_s[...] = dcur_s[...]
        return carry

    lax.fori_loop(0, users, backward, 0)
    db = finish_weights(users - 1, one)
    for part in range(4):
        finish_rows(users - 1, db, part)

    ch, cl = split(feat_s[:, width : 2 * width])
    dprec = jnp.concatenate([dprec_s[u] for u in range(users)], axis=1)
    dph, dpl = split(dprec)
    wct = split(wct_ref[...])
    dcs = split(dcand_s[...] + dot3((dph, dpl), wct, TN))
    cand_t = jnp.transpose(jnp.concatenate([cand_ref[...].astype(F32)] * (lane // cands), axis=1))
    cand_col = jnp.concatenate([cand_t[:cands, u : u + 1] for u in range(users)], axis=0)
    cand_row = jnp.transpose(jnp.broadcast_to(cand_col, (rows, lane)))[:16].astype(jnp.int32).astype(jnp.int16)
    iota = lax.broadcasted_iota(jnp.int16, (16, rows), 0)
    hot = jnp.concatenate(
        [jnp.where(cand_row - jnp.int16(k) == iota, one, zero) for k in range(0, cats, 16)], axis=0
    )
    spread = dot(hot, jnp.concatenate(dcs, axis=1))
    full_s[:cats, :] = gtab_s[...] + (spread[:, :width] + spread[:, width:])
    at = cats + fin * (fh // lane)
    full_s[at : at + hid, :] = gwb_s[...]
    full_s[at + hid : at + 2 * hid, :] = dot3((dph, dpl), (ch, cl))
    at += 2 * hid
    ones_r = jnp.ones((8, rows), BF16)
    gbias = dot(ones_r, dph, NT) + dot(ones_r, dpl, NT)
    full_s[at : at + 1, :hid] = gbias[:1]
    gao_split = split(gao_s[...])
    ones_l = jnp.ones((8, lane), BF16)
    gao_row = dot(ones_l, gao_split[0], NT) + dot(ones_l, gao_split[1], NT)
    full_s[at + 1 : at + 2, :hid] = gao_row[:1]

    half, chunk = near_ref.shape[0], near_ref.shape[1]
    for i in range(half):
        src = pl.multiple_of((place_ref[0] ^ i) * chunk, 8)
        near_ref[i] = full_s[pl.ds(src, chunk), :]
        src = pl.multiple_of((place_ref[0] ^ (half + i)) * chunk, 8)
        far_ref[i] = full_s[pl.ds(src, chunk), :]


def unpack_kernel(place_ref, near_ref, far_ref, gtab_ref, gwb_ref, gwc_ref, gbias_ref, gout_ref, gdin_ref, gdb_ref, gdo_ref, loss_ref, full_s):
    half, chunk, lane = near_ref.shape
    for i in range(half):
        dst = pl.multiple_of((place_ref[0] ^ i) * chunk, 8)
        full_s[pl.ds(dst, chunk), :] = near_ref[i]
        dst = pl.multiple_of((place_ref[0] ^ (half + i)) * chunk, 8)
        full_s[pl.ds(dst, chunk), :] = far_ref[i]
    cats = gtab_ref.shape[0]
    fin, fh = gdin_ref.shape
    hid = gwb_ref.shape[0]
    at = 0
    gtab_ref[...] = full_s[:cats, :]
    at += cats
    for j in range(fh // lane):
        gdin_ref[:, j * lane : (j + 1) * lane] = full_s[at : at + fin, :]
        at += fin
    gwb_ref[...] = full_s[at : at + hid, :]
    at += hid
    gwc_ref[...] = full_s[at : at + hid, :]
    at += hid
    gbias_ref[...] = full_s[at : at + 1, :hid]
    gout_ref[...] = full_s[at + 1 : at + 2, :hid]
    for j in range(fh // lane):
        gdb_ref[:, j * lane : (j + 1) * lane] = full_s[at + 2 + j : at + 3 + j, :]
        gdo_ref[:, j * lane : (j + 1) * lane] = full_s[at + 2 + fh // lane + j : at + 3 + fh // lane + j, :]
    k = at + 2 + 2 * (fh // lane)
    loss_ref[...] = full_s[k : k + 1, :]


def combos(bits):
    found = [0]
    for bit in bits:
        found = found + [value | (1 << bit) for value in found]
    return found


def stages_of(batch, rep):
    pair = rep.bit_length() - 1
    bits = [bit for bit in range((batch * rep).bit_length() - 1) if bit != pair]
    return pair, bits[:2], bits[2:]


def body(behav_ids, lengths, cand_ids, labels, item_table, att_behav, att_cand, att_bias, att_out, dense_in, dense_bias, dense_out):
    batch = lax.axis_size("batch")
    rep = lax.axis_size("rep")
    devices = batch * rep
    users, seq = behav_ids.shape
    cands = cand_ids.shape[1]
    rows = users * cands
    cats, width = item_table.shape
    hid = att_behav.shape[1]
    fin, fh = dense_in.shape
    lane = 128
    tail = 3 + 2 * (fh // lane)
    need = cats + fin * (fh // lane) + 2 * hid + tail
    pair, spread, rest = stages_of(batch, rep)
    half = 1 << len(spread)
    chunk = 8 * math.ceil(need / (8 * 2 * half))
    me = lax.axis_index("batch") * rep + lax.axis_index("rep")
    place = sum(((me >> bit) & 1) << k for k, bit in enumerate(spread + [pair])).astype(jnp.int32)[None]

    smem = pl.BlockSpec(memory_space=pltpu.SMEM)
    vmem = pl.BlockSpec(memory_space=pltpu.VMEM)
    near, far = pl.pallas_call(
        local_kernel,
        in_specs=[smem, smem] + [vmem] * 11,
        out_specs=[vmem, vmem],
        out_shape=[pltpu.VMEM((half, chunk, lane), F32)] * 2,
        scratch_shapes=[
            pltpu.VMEM((cats, 2 * width), BF16),
            pltpu.VMEM((hid, lane), F32),
            pltpu.VMEM((width, 3 * hid), BF16),
            pltpu.VMEM((users, hid, cands), F32),
            pltpu.VMEM((rows, lane), F32),
            pltpu.VMEM((seq, users), F32),
            pltpu.VMEM((users, hid, seq), F32),
            pltpu.VMEM((hid, seq), F32),
            pltpu.VMEM((hid, seq), F32),
            pltpu.VMEM((users, seq, 2 * width), BF16),
            pltpu.VMEM((seq, 2 * width), BF16),
            pltpu.VMEM((cands, seq), F32),
            pltpu.VMEM((users, 6 * cands, seq), BF16),
            pltpu.VMEM((rows, fin), F32),
            pltpu.VMEM((users, 6 * cands, width), BF16),
            pltpu.VMEM((users, cands, seq), F32),
            pltpu.VMEM((users, hid, cands), F32),
            pltpu.VMEM((hid, seq), F32),
            pltpu.VMEM((hid, seq), F32),
            pltpu.VMEM((cats, width), F32),
            pltpu.VMEM((hid, width), F32),
            pltpu.VMEM((hid, lane), F32),
            pltpu.VMEM((rows, width), F32),
            pltpu.VMEM((2 * half * chunk, lane), F32),
        ],
        name="local_step",
    )(
        place, lengths, behav_ids, cand_ids, labels, item_table, att_behav.T, att_cand.T, att_bias[None],
        att_out[None], dense_in, dense_bias[None], dense_out[None],
    )

    def swap(value, distance):
        return lax.ppermute(value, AXES, [(d, d ^ distance) for d in range(devices)])

    steps = combos(spread)
    x = near.reshape(half * chunk, lane) + swap(far.reshape(half * chunk, lane), 1 << pair)
    x = x.reshape(half, chunk, lane)
    got = [swap(x[i], step) for i, step in enumerate(steps) if step]
    x = x[0]
    for piece in got:
        x = x + piece
    reach = 0
    for bit in rest:
        reach = reach | (1 << bit)
        x = x + swap(x, reach)
    x = x * (1.0 / (rows * devices))
    near = jnp.concatenate([x] + [swap(x, step) for step in steps if step], axis=0)
    far = swap(near, 1 << pair)
    near, far = (
        pltpu.with_memory_space_constraint(side.reshape(half, chunk, lane), pltpu.VMEM) for side in (near, far)
    )
    outs = pl.pallas_call(
        unpack_kernel,
        in_specs=[smem, vmem, vmem],
        out_specs=[vmem] * 9,
        out_shape=[
            jax.ShapeDtypeStruct(shape, F32)
            for shape in (
                (cats, width), (hid, width), (hid, width), (1, hid), (1, hid), (fin, fh), (1, fh), (1, fh), (1, lane),
            )
        ],
        scratch_shapes=[pltpu.VMEM((2 * half * chunk, lane), F32)],
        name="unpack",
    )(place, near, far)
    gtab, gwb, gwc, gbias, gout, gdin, gdb, gdo, loss = outs
    return gtab, gwb.T, gwc.T, gbias[0], gout[0], gdin, gdb[0], gdo[0], loss[0, 0]


def solution(mesh):
    split_users = P(("batch", "rep"))
    placed = (split_users,) * 4 + (P(),) * 8
    return jax.shard_map(body, mesh=mesh, in_specs=placed, out_specs=(P(),) * 9, check_vma=False)
```

```python
import math

import jax
import jax.numpy as jnp
from jax import lax
from jax.experimental import pallas as pl
from jax.experimental.pallas import tpu as pltpu
from jax.sharding import PartitionSpec as P

AXES = ("batch", "rep")
F32 = jnp.float32
BF16 = jnp.bfloat16
NN = (((1,), (0,)), ((), ()))
NT = (((1,), (1,)), ((), ()))
TN = (((0,), (0,)), ((), ()))


def split(x):
    high = x.astype(BF16)
    return high, (x - high.astype(F32)).astype(BF16)


def dot(a, b, dims=NN):
    return lax.dot_general(a, b, dims, preferred_element_type=F32)


def dot3(a, b, dims=NN):
    (ah, al), (bh, bl) = a, b
    return dot(ah, bh, dims) + (dot(ah, bl, dims) + dot(al, bh, dims))


def local_kernel(
    place_ref, lens_ref, idlist_ref, ids_ref, cand_ref, label_ref, table_ref, wbt_ref, wct_ref, bias_ref, out_ref,
    din_ref, dbias_ref, dout_ref,
    near_ref, far_ref,
    table_s, aob_s, wside_s, prec_s, wide_s, wnext_s, lin_s, rows_s, preb_s, pbcur_s, pbnext_s, b_s, bnext_s, raw_s, scst_s,
    feat_s, dpst_s, ds_s, dprec_s, dcur_s, dprev_s, gtab_s, gwb_s, gao_s, dcand_s, full_s,
):
    users, seq = ids_ref.shape
    cats, width = table_ref.shape
    hid = wbt_ref.shape[0]
    cands = cand_ref.shape[1]
    rows = users * cands
    lane = 128
    tiles = hid // 8
    pad = 2 * cands
    one, zero = BF16(1), BF16(0)

    th, tl = split(table_ref[...])
    table_s[:, :width] = th
    table_s[:, width:] = tl
    wbh, wbl = split(0.5 * wbt_ref[...])
    wbhh = jnp.concatenate([wbh, wbh], axis=1)
    wch, wcl = split(0.5 * wct_ref[...])
    wh, wl = split(jnp.transpose(wbt_ref[...]))
    wside_s[:, :hid] = wh
    wside_s[:, hid : 2 * hid] = wh
    wside_s[:, 2 * hid :] = wl
    bias_col = jnp.transpose(jnp.broadcast_to(bias_ref[...], (8, hid)))[:, :1]
    ao_col = jnp.transpose(jnp.broadcast_to(out_ref[...], (8, hid)))[:, :1]
    aob_s[...] = jnp.broadcast_to(ao_col, (hid, lane))

    cand_t = jnp.transpose(jnp.concatenate([cand_ref[...].astype(F32)] * (lane // cands), axis=1))
    cand_col = jnp.concatenate([cand_t[:cands, u : u + 1] for u in range(users)], axis=0)
    label_t = jnp.transpose(jnp.concatenate([label_ref[...].astype(F32)] * (lane // cands), axis=1))
    label = jnp.concatenate([label_t[:cands, u : u + 1] for u in range(users)], axis=0)

    def onehot(col, n):
        wide = jnp.broadcast_to(col, (n, lane)).astype(jnp.int32).astype(jnp.int16)
        iota = lax.broadcasted_iota(jnp.int16, (n, lane), 1)
        return jnp.concatenate(
            [jnp.where(wide - jnp.int16(lane * k) == iota, one, zero) for k in range(cats // lane)], axis=1
        )

    pair = dot(onehot(cand_col, rows), table_s[...])
    cand = pair[:, :width] + pair[:, width:]
    cpair = pair.astype(BF16)
    prec_all = (
        dot(jnp.concatenate([wch, wch], axis=1), cpair, NT) + dot(wcl, cpair[:, :width], NT) + 0.5 * bias_col
    )
    for u in range(users):
        prec_s[u] = prec_all[:, u * cands : (u + 1) * cands]
    lin_row = jnp.broadcast_to(jnp.sum(prec_all * ao_col, axis=0, keepdims=True), (lane, rows))
    lin_s[...] = jnp.transpose(lin_row)
    feat_s[:, width : 2 * width] = cand

    iota_s = lax.broadcasted_iota(jnp.int32, (cands, seq), 1)
    group = 4

    def fetch(u, at, count):
        for r in range(at, at + count):
            rows_s[r : r + 1, :] = table_ref[pl.ds(idlist_ref[u, r], 1), :]

    def halves():
        high, low = split(rows_s[...])
        bnext_s[:, :width] = high
        bnext_s[:, width:] = low

    def widen(u, p):
        wnext_s[p] = jnp.broadcast_to(prec_s[u, :, p : p + 1], (hid, lane))

    def project():
        b = bnext_s[...]
        pbnext_s[...] = dot(wbhh, b, NT) + dot(wbl, b[:, :width], NT)

    fetch(0, 0, seq)
    halves()
    project()
    for p in range(cands):
        widen(0, p)

    def forward(u, carry):
        b_s[u] = bnext_s[...]
        pb_all = pbnext_s[...]
        preb_s[u] = pb_all
        pbcur_s[...] = pb_all
        wide_s[u] = wnext_s[...]
        following = jnp.minimum(u + 1, users - 1)
        lin = jnp.zeros((8, seq), F32)
        for g0 in range(0, cands, group):
            if g0 < cands // 2:
                fetch(following, g0 * seq * 2 // cands, group * seq * 2 // cands)
            if g0 == cands // 2:
                halves()
                project()
            for j in range(group):
                widen(following, g0 + j)
            accs = [jnp.zeros((8, seq), F32) for _ in range(group)]
            for t in range(tiles):
                sl = slice(8 * t, 8 * t + 8)
                pb = pbcur_s[sl, :]
                ao = aob_s[sl, :]
                ao = jnp.concatenate([ao] * (seq // lane), axis=1)
                if g0 == 0:
                    lin = lin + ao * pb
                for j in range(group):
                    pc = wide_s[u, g0 + j, sl, :]
                    v = pb + jnp.concatenate([pc] * (seq // lane), axis=1)
                    accs[j] = accs[j] + (ao * v) * jnp.tanh(v)
            for j in range(group):
                raw_s[g0 + j : g0 + j + 1, :] = jnp.sum(accs[j] + lin, axis=0, keepdims=True)
        live = (iota_s < lens_ref[u]).astype(F32)
        base = pl.multiple_of(u * cands, cands)
        lin_c = lin_s[pl.ds(base, cands), :]
        sc = (raw_s[...] + jnp.concatenate([lin_c] * (seq // lane), axis=1)) * live
        sh, sl_ = split(sc)
        lh = live.astype(BF16)
        scst_s[u, :cands, :] = sh
        scst_s[u, cands:pad, :] = lh
        scst_s[u, pad : pad + cands, :] = sl_
        scst_s[u, pad + cands : 2 * pad, :] = jnp.zeros((cands, seq), BF16)
        scst_s[u, 2 * pad : 2 * pad + cands, :] = sh
        scst_s[u, 2 * pad + cands :, :] = lh
        return carry

    lax.fori_loop(0, users, forward, 0)

    for u in range(users):
        b = b_s[u]
        wide = dot(scst_s[u, :pad, :], b)
        mix = wide[:, :width] + wide[:, width:] + dot(scst_s[u, pad : 2 * pad, :], b[:, :width])
        feat_s[u * cands : (u + 1) * cands, :width] = mix[:cands] * (1.0 / seq)
        avg = mix[cands : cands + 1] / lens_ref[u].astype(F32)
        feat_s[u * cands : (u + 1) * cands, 3 * width :] = jnp.broadcast_to(avg, (cands, width))

    pooled = feat_s[:, :width]
    cand = feat_s[:, width : 2 * width]
    feat_s[:, 2 * width : 3 * width] = pooled * cand
    fsp = split(feat_s[...])
    dsp = split(din_ref[...])
    z = 0.5 * (dot3(fsp, dsp) + dbias_ref[...])
    tz = jnp.tanh(z)
    q = 1.0 + tz
    hidden = z * q
    logit = jnp.sum(hidden * dout_ref[...], axis=1, keepdims=True)
    loss_rows = jnp.maximum(logit, 0.0) + jnp.log1p(jnp.exp(-jnp.abs(logit))) - label * logit
    dlogit = 0.5 * (1.0 + jnp.tanh(0.5 * logit)) - label
    dz = (dlogit * dout_ref[...]) * (0.5 * (q + hidden * (1.0 - tz)))
    zsp = split(dz)
    dfeat = dot3(zsp, dsp, NT)
    gdin = dot3(fsp, zsp, TN)
    gdout = jnp.sum(dlogit * hidden, axis=0, keepdims=True)
    gdbias = jnp.sum(dz, axis=0, keepdims=True)
    loss = jnp.sum(loss_rows)
    dmix = dfeat[:, 2 * width : 3 * width]
    dpool = (dfeat[:, :width] + dmix * cand) * (1.0 / seq)
    dcand_s[...] = dfeat[:, width : 2 * width] + dmix * pooled
    fin, fh = gdin.shape
    for j in range(fh // lane):
        full_s[cats + j * fin : cats + (j + 1) * fin, :] = gdin[:, j * lane : (j + 1) * lane]
    at = cats + fin * (fh // lane) + 2 * hid
    full_s[at:, :] = jnp.zeros((full_s.shape[0] - at, lane), F32)
    for j in range(fh // lane):
        full_s[at + 2 + j : at + 3 + j, :] = gdbias[:, j * lane : (j + 1) * lane]
        full_s[at + 2 + fh // lane + j : at + 3 + fh // lane + j, :] = gdout[:, j * lane : (j + 1) * lane]
    k = 2 + 2 * (fh // lane)
    full_s[at + k : at + k + 1, :] = jnp.full((1, lane), loss, F32)

    first = lax.broadcasted_iota(jnp.int32, (cands, width), 0) == 0
    for u in range(users):
        part = jnp.sum(dfeat[u * cands : (u + 1) * cands, 3 * width :], axis=0, keepdims=True)
        davg = jnp.where(first, part / lens_ref[u].astype(F32), 0.0)
        dh, dl = split(jnp.concatenate([dpool[u * cands : (u + 1) * cands], davg], axis=0))
        dpst_s[u, :pad, :] = dh
        dpst_s[u, pad : 2 * pad, :] = dh
        dpst_s[u, 2 * pad :, :] = dl
        b = b_s[u]
        live = (iota_s < lens_ref[u]).astype(F32)
        grad = dot(jnp.concatenate([dh[:cands], dh[:cands]], axis=1), b, NT) + dot(dl[:cands], b[:, :width], NT)
        ds_s[u] = grad * live

    gtab_s[...] = jnp.zeros_like(gtab_s)
    gwb_s[...] = jnp.zeros_like(gwb_s)
    gao_s[...] = jnp.zeros_like(gao_s)
    dprev_s[...] = jnp.zeros_like(dprev_s)
    lane_i = lax.broadcasted_iota(jnp.int32, (8, lane), 1)
    block = cats // 4

    def finish_weights(u, keep):
        ph, pl_ = split(dprev_s[...])
        b = b_s[u]
        wide = dot(ph, b)
        gwb_s[...] += wide[:, :width] + wide[:, width:] + dot(pl_, b[:, :width])
        db = dot(wside_s[...], jnp.concatenate([ph, pl_, ph], axis=0))
        db = db + dot(dpst_s[u] * keep, scst_s[u], TN)
        return jnp.concatenate(split(db), axis=0)

    def finish_rows(u, db, part):
        row = jnp.broadcast_to(ids_ref[pl.ds(u, 1), :], (16, seq)).astype(jnp.int16)
        iota = lax.broadcasted_iota(jnp.int16, (16, seq), 0)
        start = part * block
        hot = jnp.concatenate(
            [jnp.where(row - jnp.int16(start + k) == iota, one, zero) for k in range(0, block, 16)], axis=0
        )
        spread = dot(hot, db, NT)
        gtab_s[start : start + block, :] += spread[:, :width] + spread[:, width:]

    def backward(u, carry):
        prev = jnp.maximum(u - 1, 0)
        keep = (u > 0).astype(F32).astype(BF16)
        db = None
        for t in range(tiles):
            if t == 0:
                db = finish_weights(prev, keep)
            if t >= 2 and t % 2 == 0:
                finish_rows(prev, db, t // 2 - 1)
            sl = slice(8 * t, 8 * t + 8)
            pb = preb_s[u, sl, :]
            acc = jnp.zeros((8, seq), F32)
            gao = gao_s[sl, :]
            dpc = jnp.zeros((8, lane), F32)
            for p in range(cands):
                grad = ds_s[u, p : p + 1, :]
                pc = wide_s[u, p, sl, :]
                v = pb + jnp.concatenate([pc] * (seq // lane), axis=1)
                th_ = jnp.tanh(v)
                q_ = 1.0 + th_
                act = v * q_
                gd = (q_ + act * (1.0 - th_)) * grad
                acc = acc + gd
                ad = act * grad
                gao = gao + (ad[:, :lane] + ad[:, lane:])
                red = jnp.sum(gd[:, :lane] + gd[:, lane:], axis=1, keepdims=True)
                dpc = jnp.where(lane_i == p, red, dpc)
            gao_s[sl, :] = gao
            half = 0.5 * aob_s[sl, :]
            dprec_s[u, sl, :] = (dpc * half)[:, :cands]
            dcur_s[sl, :] = acc * jnp.concatenate([half] * (seq // lane), axis=1)
        dprev_s[...] = dcur_s[...]
        return carry

    lax.fori_loop(0, users, backward, 0)
    db = finish_weights(users - 1, one)
    for part in range(4):
        finish_rows(users - 1, db, part)

    ch, cl = split(feat_s[:, width : 2 * width])
    dprec = jnp.concatenate([dprec_s[u] for u in range(users)], axis=1)
    dph, dpl = split(dprec)
    wct = split(wct_ref[...])
    dcs = split(dcand_s[...] + dot3((dph, dpl), wct, TN))
    cand_t = jnp.transpose(jnp.concatenate([cand_ref[...].astype(F32)] * (lane // cands), axis=1))
    cand_col = jnp.concatenate([cand_t[:cands, u : u + 1] for u in range(users)], axis=0)
    cand_row = jnp.transpose(jnp.broadcast_to(cand_col, (rows, lane)))[:16].astype(jnp.int32).astype(jnp.int16)
    iota = lax.broadcasted_iota(jnp.int16, (16, rows), 0)
    hot = jnp.concatenate(
        [jnp.where(cand_row - jnp.int16(k) == iota, one, zero) for k in range(0, cats, 16)], axis=0
    )
    spread = dot(hot, jnp.concatenate(dcs, axis=1))
    full_s[:cats, :] = gtab_s[...] + (spread[:, :width] + spread[:, width:])
    at = cats + fin * (fh // lane)
    full_s[at : at + hid, :] = gwb_s[...]
    full_s[at + hid : at + 2 * hid, :] = dot3((dph, dpl), (ch, cl))
    at += 2 * hid
    ones_r = jnp.ones((8, rows), BF16)
    gbias = dot(ones_r, dph, NT) + dot(ones_r, dpl, NT)
    full_s[at : at + 1, :hid] = gbias[:1]
    gao_split = split(gao_s[...])
    ones_l = jnp.ones((8, lane), BF16)
    gao_row = dot(ones_l, gao_split[0], NT) + dot(ones_l, gao_split[1], NT)
    full_s[at + 1 : at + 2, :hid] = gao_row[:1]

    half, chunk = near_ref.shape[0], near_ref.shape[1]
    for i in range(half):
        src = pl.multiple_of((place_ref[0] ^ i) * chunk, 8)
        near_ref[i] = full_s[pl.ds(src, chunk), :]
        src = pl.multiple_of((place_ref[0] ^ (half + i)) * chunk, 8)
        far_ref[i] = full_s[pl.ds(src, chunk), :]


def unpack_kernel(place_ref, near_ref, far_ref, gtab_ref, gwb_ref, gwc_ref, gbias_ref, gout_ref, gdin_ref, gdb_ref, gdo_ref, loss_ref, full_s):
    half, chunk, lane = near_ref.shape
    for i in range(half):
        dst = pl.multiple_of((place_ref[0] ^ i) * chunk, 8)
        full_s[pl.ds(dst, chunk), :] = near_ref[i]
        dst = pl.multiple_of((place_ref[0] ^ (half + i)) * chunk, 8)
        full_s[pl.ds(dst, chunk), :] = far_ref[i]
    cats = gtab_ref.shape[0]
    fin, fh = gdin_ref.shape
    hid = gwb_ref.shape[0]
    at = 0
    gtab_ref[...] = full_s[:cats, :]
    at += cats
    for j in range(fh // lane):
        gdin_ref[:, j * lane : (j + 1) * lane] = full_s[at : at + fin, :]
        at += fin
    gwb_ref[...] = full_s[at : at + hid, :]
    at += hid
    gwc_ref[...] = full_s[at : at + hid, :]
    at += hid
    gbias_ref[...] = full_s[at : at + 1, :hid]
    gout_ref[...] = full_s[at + 1 : at + 2, :hid]
    for j in range(fh // lane):
        gdb_ref[:, j * lane : (j + 1) * lane] = full_s[at + 2 + j : at + 3 + j, :]
        gdo_ref[:, j * lane : (j + 1) * lane] = full_s[at + 2 + fh // lane + j : at + 3 + fh // lane + j, :]
    k = at + 2 + 2 * (fh // lane)
    loss_ref[...] = full_s[k : k + 1, :]


def combos(bits):
    found = [0]
    for bit in bits:
        found = found + [value | (1 << bit) for value in found]
    return found


def stages_of(batch, rep):
    pair = rep.bit_length() - 1
    bits = [bit for bit in range((batch * rep).bit_length() - 1) if bit != pair]
    return pair, bits[:2], bits[2:]


def body(behav_ids, lengths, cand_ids, labels, item_table, att_behav, att_cand, att_bias, att_out, dense_in, dense_bias, dense_out):
    batch = lax.axis_size("batch")
    rep = lax.axis_size("rep")
    devices = batch * rep
    users, seq = behav_ids.shape
    cands = cand_ids.shape[1]
    rows = users * cands
    cats, width = item_table.shape
    hid = att_behav.shape[1]
    fin, fh = dense_in.shape
    lane = 128
    tail = 3 + 2 * (fh // lane)
    need = cats + fin * (fh // lane) + 2 * hid + tail
    pair, spread, rest = stages_of(batch, rep)
    half = 1 << len(spread)
    chunk = 8 * math.ceil(need / (8 * 2 * half))
    me = lax.axis_index("batch") * rep + lax.axis_index("rep")
    place = sum(((me >> bit) & 1) << k for k, bit in enumerate(spread + [pair])).astype(jnp.int32)[None]

    smem = pl.BlockSpec(memory_space=pltpu.SMEM)
    vmem = pl.BlockSpec(memory_space=pltpu.VMEM)
    near, far = pl.pallas_call(
        local_kernel,
        in_specs=[smem, smem, smem] + [vmem] * 11,
        out_specs=[vmem, vmem],
        out_shape=[pltpu.VMEM((half, chunk, lane), F32)] * 2,
        scratch_shapes=[
            pltpu.VMEM((cats, 2 * width), BF16),
            pltpu.VMEM((hid, lane), F32),
            pltpu.VMEM((width, 3 * hid), BF16),
            pltpu.VMEM((users, hid, cands), F32),
            pltpu.VMEM((users, cands, hid, lane), F32),
            pltpu.VMEM((cands, hid, lane), F32),
            pltpu.VMEM((rows, lane), F32),
            pltpu.VMEM((seq, width), F32),
            pltpu.VMEM((users, hid, seq), F32),
            pltpu.VMEM((hid, seq), F32),
            pltpu.VMEM((hid, seq), F32),
            pltpu.VMEM((users, seq, 2 * width), BF16),
            pltpu.VMEM((seq, 2 * width), BF16),
            pltpu.VMEM((cands, seq), F32),
            pltpu.VMEM((users, 6 * cands, seq), BF16),
            pltpu.VMEM((rows, fin), F32),
            pltpu.VMEM((users, 6 * cands, width), BF16),
            pltpu.VMEM((users, cands, seq), F32),
            pltpu.VMEM((users, hid, cands), F32),
            pltpu.VMEM((hid, seq), F32),
            pltpu.VMEM((hid, seq), F32),
            pltpu.VMEM((cats, width), F32),
            pltpu.VMEM((hid, width), F32),
            pltpu.VMEM((hid, lane), F32),
            pltpu.VMEM((rows, width), F32),
            pltpu.VMEM((2 * half * chunk, lane), F32),
        ],
        name="local_step",
    )(
        place, lengths, behav_ids, behav_ids, cand_ids, labels, item_table, att_behav.T, att_cand.T, att_bias[None],
        att_out[None], dense_in, dense_bias[None], dense_out[None],
    )

    def swap(value, distance):
        return lax.ppermute(value, AXES, [(d, d ^ distance) for d in range(devices)])

    steps = combos(spread)
    x = near.reshape(half * chunk, lane) + swap(far.reshape(half * chunk, lane), 1 << pair)
    x = x.reshape(half, chunk, lane)
    got = [swap(x[i], step) for i, step in enumerate(steps) if step]
    x = x[0]
    for piece in got:
        x = x + piece
    reach = 0
    for bit in rest:
        reach = reach | (1 << bit)
        x = x + swap(x, reach)
    x = x * (1.0 / (rows * devices))
    near = jnp.concatenate([x] + [swap(x, step) for step in steps if step], axis=0)
    far = swap(near, 1 << pair)
    near, far = (
        pltpu.with_memory_space_constraint(side.reshape(half, chunk, lane), pltpu.VMEM) for side in (near, far)
    )
    outs = pl.pallas_call(
        unpack_kernel,
        in_specs=[smem, vmem, vmem],
        out_specs=[vmem] * 9,
        out_shape=[
            jax.ShapeDtypeStruct(shape, F32)
            for shape in (
                (cats, width), (hid, width), (hid, width), (1, hid), (1, hid), (fin, fh), (1, fh), (1, fh), (1, lane),
            )
        ],
        scratch_shapes=[pltpu.VMEM((2 * half * chunk, lane), F32)],
        name="unpack",
    )(place, near, far)
    gtab, gwb, gwc, gbias, gout, gdin, gdb, gdo, loss = outs
    return gtab, gwb.T, gwc.T, gbias[0], gout[0], gdin, gdb[0], gdo[0], loss[0, 0]


def solution(mesh):
    split_users = P(("batch", "rep"))
    placed = (split_users,) * 4 + (P(),) * 8
    return jax.shard_map(body, mesh=mesh, in_specs=placed, out_specs=(P(),) * 9, check_vma=False)
```
